32 devices in a mesh: dp: 4 (over z), expert: 8 (over y, x, core).
Axes of the slice: x: 2, y: 2, z: 4, core: 2. Of those that a mesh axis runs over, the one named last changes fastest.
Arguments:
- tokens: bfloat16 [32768, 2080], P(('dp', 'expert')), may hold values from -6 to 6
- router_logits: bfloat16 [32768, 2048], P(('dp', 'expert')), may hold values from -300 to 300
- gate_grad: float32 [32768], P(('dp', 'expert')), may hold values from -6 to 6
- expert_index: int32 [32768, 1], P(('dp', 'expert')), may hold values from 0 to 2047
- keep_mask: int32 [2048], replicated, may hold values 0 or 1
Outputs:
- router_grad: float32 [2048, 2080], P('expert', 'dp')
The draws below stay inside these ranges and needn't reach their ends.
All inputs are finite; a program needn't handle non-finite values.
Results may differ from the reference program's by a relative error of at most 0.0003.
Values sent between devices are 32-bit elements; how exact they have to be, the bound alone decides.
No kernel may reach another device: no remote copies, remote signals or barrier semaphores. Data moves between devices by JAX's collectives and lax.ppermute only.
A program may use at most 128 MiB of HBM per device.

```python
import math
import jax
import jax.numpy as jnp
from jax import lax

D = 2080
E = 2048
TOKENS = 32768


def draw_router_logits(key, part):
    first_key, second_key, third_key = jax.random.split(jax.random.fold_in(key, 17), 3)
    values = 2.0 * jax.random.normal(first_key, (TOKENS, E), jnp.float32)
    return values.astype(jnp.bfloat16)


def touch_ends(array, stream_key, least, high):
    longest = array.shape.index(max(array.shape))
    spots = []
    for shift in (0, 1):
        where = [jax.random.randint(jax.random.fold_in(stream_key, axis), (), 0, length) for axis, length in enumerate(array.shape)]
        where[longest] = (where[longest] + shift) % array.shape[longest]
        spots.append(tuple(where))
    return array.at[spots[0]].set(least).at[spots[1]].set(high)


def level_of(key, extent, shards, smallest, top_value):
    def one(position, shards_of):
        heights = jax.random.uniform(jax.random.fold_in(jax.random.fold_in(key, 6), position), (shards_of,), jnp.float32, smallest / len(shards), top_value / len(shards))
        return jnp.repeat(jnp.exp(heights), extent[position] // shards_of).reshape((-1,) + (1,) * (len(extent) - position - 1))

    gain = one(*shards[0])
    for cut in shards[1:]:
        gain = gain * one(*cut)
    return gain


def different_ones(rng, rows, amount, top, lift):
    order = jax.random.permutation(jax.random.fold_in(rng, 1), amount)
    boost = order
    for power in range(3):
        boost = boost * boost // amount
    boost = boost * lift // amount
    lots = jax.random.randint(jax.random.fold_in(rng, 2), (rows, amount), 0, 4096) + boost
    fixed_rows = jax.random.permutation(jax.random.fold_in(rng, 3), rows)[jnp.arange(amount) % rows]
    lots = jnp.where(jnp.arange(rows)[:, None] == fixed_rows[None, :], 1 << 14, lots)
    priority = lots * amount + jnp.arange(amount)
    return lax.top_k(priority.astype(jnp.int32), top)[1].astype(jnp.int32)


def bell_draw(stream_key, extent, width, bound, cuts=(), kind=jnp.bfloat16):
    result = jax.random.normal(stream_key, extent, jnp.float32) * width
    if len(cuts) > 0:
        result = level_of(stream_key, extent, cuts, -0.22, 0.18) * result
    return jnp.clip(result, min=-bound, max=bound).astype(kind)


def setup_inputs(seed: int = 0) -> dict:
    arg_keys = jax.random.split(jax.random.key(seed), 6)
    tokens = bell_draw(arg_keys[0], (TOKENS, D), 1.0, 6.0, ((0, 32),))
    router_logits = draw_router_logits(jax.random.fold_in(arg_keys[5], 71), 0)
    gate_grad = bell_draw(arg_keys[2], (TOKENS,), 1.0, 6.0, ((0, 32),), jnp.float32)
    expert_index = different_ones(arg_keys[3], TOKENS, E, 1, 8)
    keep_mask = touch_ends((jax.random.randint(arg_keys[4], (E,), 0, 8) < 7).astype(jnp.int32), jax.random.fold_in(arg_keys[4], 1), 0, 1)
    return dict(tokens=tokens, router_logits=router_logits, gate_grad=gate_grad, expert_index=expert_index, keep_mask=keep_mask)


def logit_gradient(logit_block, gate_block, routed_block, aux_cost, kept_cols):
    scores = logit_block.astype(jnp.float32)
    row_peak = jnp.max(scores, axis=1, keepdims=True)
    weights = jnp.exp(scores - row_peak)
    router_probs = weights / jnp.sum(weights, axis=1, keepdims=True)
    columns = lax.broadcasted_iota(jnp.int32, scores.shape, 1)
    chosen = columns == routed_block[:, None]
    top_prob = jnp.sum(jnp.where(chosen, router_probs, 0.0), axis=1)
    spread = jnp.dot(router_probs, aux_cost, precision=lax.Precision.HIGHEST)
    gate_part = (gate_block * top_prob)[:, None] * (chosen.astype(jnp.float32) - router_probs)
    aux_part = router_probs * (aux_cost[None, :] - spread[:, None])
    return kept_cols[None, :] * (gate_part + aux_part)


def reference(tokens, router_logits, gate_grad, expert_index, keep_mask):
    routed = expert_index[:, 0].astype(jnp.int32)
    total_tokens = tokens.shape[0]
    expert_total = router_logits.shape[1]
    counts = jax.ops.segment_sum(jnp.ones((total_tokens,), jnp.int32), routed, num_segments=expert_total)
    aux_cost = counts.astype(jnp.float32) * (expert_total / total_tokens)
    kept_cols = keep_mask.astype(jnp.float32)
    block_rows = math.gcd(total_tokens, 4096)
    offsets = jnp.arange(total_tokens // block_rows, dtype=jnp.int32) * block_rows

    def advance(running, offset):
        token_block = lax.dynamic_slice_in_dim(tokens, offset, block_rows, 0)
        logit_block = lax.dynamic_slice_in_dim(router_logits, offset, block_rows, 0)
        gate_block = lax.dynamic_slice_in_dim(gate_grad, offset, block_rows, 0)
        routed_block = lax.dynamic_slice_in_dim(routed, offset, block_rows, 0)
        grad_block = logit_gradient(logit_block, gate_block, routed_block, aux_cost, kept_cols)
        running = running + lax.dot_general(grad_block.astype(jnp.float32), token_block.astype(jnp.float32), (((0,), (0,)), ((), ())), precision=lax.Precision.HIGHEST, preferred_element_type=jnp.float32)
        return running, None

    start_value = jnp.zeros((expert_total, tokens.shape[1]), jnp.float32)
    final, unused = lax.scan(advance, start_value, offsets)
    return final
```

```python
import functools

import jax
import jax.numpy as jnp
from jax import lax
from jax.experimental import pallas as pl
from jax.experimental.pallas import tpu as pltpu
from jax.sharding import PartitionSpec as P


LANES = 128
SUBLANES = 8


def widths():
    return lax.axis_size("dp"), lax.axis_size("expert")


def local_counts(routed, expert_total):
    high = routed // LANES
    low = routed % LANES
    rows = expert_total // LANES
    high_hot = (high[:, None] == jnp.arange(rows)[None, :]).astype(jnp.bfloat16)
    low_hot = (low[:, None] == jnp.arange(LANES)[None, :]).astype(jnp.bfloat16)
    found = lax.dot_general(
        high_hot, low_hot, (((0,), (0,)), ((), ())), preferred_element_type=jnp.float32
    )
    return found.astype(jnp.int32)


def exchange(value, axis, mask):
    size = lax.axis_size(axis)
    return lax.ppermute(value, axis, [(i, i ^ mask) for i in range(size)])


def global_counts(counts):
    dp_width, expert_width = widths()
    counts = counts + exchange(counts, "expert", 1)
    counts = sum((exchange(counts, "expert", m) for m in range(2, expert_width, 2)), counts)
    return sum((exchange(counts, "dp", m) for m in range(1, dp_width)), counts)


def tiles(width):
    return [slice(k, k + LANES) for k in range(0, width, LANES)]


def down(row):
    return jnp.broadcast_to(row, (LANES, LANES)).T


def across(column):
    return column.T[:1, :]


def total_of(parts):
    return jnp.broadcast_to(jnp.sum(parts, axis=1, keepdims=True), parts.shape)


def lane_places(shape):
    return lax.broadcasted_iota(jnp.int32, shape, 1)


def softmax_kernel(logits_ref, routed_ref, gate_ref, peak_ref, inverse_ref, scale_ref):
    row = pl.ds(pl.program_id(0), 1)
    spans = tiles(logits_ref.shape[1])
    peak = None
    for lanes in spans:
        scores = logits_ref[:, lanes].astype(jnp.float32)
        peak = scores if peak is None else jnp.maximum(peak, scores)
    peak = jnp.broadcast_to(jnp.max(peak, axis=1, keepdims=True), peak.shape)
    routed = down(routed_ref[row, :]) - lane_places(peak.shape)
    total = jnp.zeros_like(peak)
    top = jnp.zeros_like(peak)
    for lanes in spans:
        weights = jnp.exp(logits_ref[:, lanes].astype(jnp.float32) - peak)
        total += weights
        top += jnp.where(routed == lanes.start, weights, 0.0)
    inverse = 1.0 / across(total_of(total))
    peak_ref[row, :] = across(peak)
    inverse_ref[row, :] = inverse
    scale_ref[row, :] = across(total_of(top)) * inverse * gate_ref[row, :]


def softmax(router_logits, routed, gate_grad):
    rows, experts = router_logits.shape
    blocks = rows // LANES
    wide = pl.BlockSpec((LANES, experts), lambda i: (i, 0))
    thin = pl.BlockSpec((blocks, LANES), lambda i: (0, 0))
    return pl.pallas_call(
        softmax_kernel,
        grid=(blocks,),
        in_specs=[wide, thin, thin],
        out_specs=[thin] * 3,
        out_shape=[jax.ShapeDtypeStruct((blocks, LANES), jnp.float32)] * 3,
        cost_estimate=pl.CostEstimate(
            flops=20 * rows * experts, bytes_accessed=2 * rows * experts, transcendentals=rows * experts
        ),
        name="softmax",
    )(router_logits, routed, gate_grad)


def grad_block(unit, index, refs, probs_ref, store):
    logits_ref, routed_ref, peak_ref, inverse_ref, scale_ref, counts_ref, keep_ref = refs
    row = pl.ds(index, 1)
    spans = tiles(logits_ref.shape[1])
    peak = down(peak_ref[row, :])
    inverse = down(inverse_ref[row, :])
    spread = jnp.zeros_like(peak)
    for lanes in spans:
        aux = counts_ref[:, lanes].astype(jnp.float32) * unit
        probs = jnp.exp(logits_ref[:, lanes].astype(jnp.float32) - peak) * inverse
        probs_ref[:, lanes] = probs
        spread += probs * aux
    spread = total_of(spread)
    scale = down(scale_ref[row, :])
    routed = down(routed_ref[row, :]) - lane_places(spread.shape)
    for lanes in spans:
        aux = counts_ref[:, lanes].astype(jnp.float32) * unit
        probs = probs_ref[:, lanes]
        chosen = jnp.where(routed == lanes.start, 1.0, 0.0)
        grad = scale * (chosen - probs) + probs * (aux - spread)
        grad = keep_ref[:, lanes].astype(jnp.float32) * grad
        high = grad.astype(jnp.bfloat16)
        low = (grad - high.astype(jnp.float32)).astype(jnp.bfloat16)
        store(lanes, high, low)


def grad_kernel(unit, *refs):
    high_ref, low_ref, probs_ref = refs[-3:]

    def store(lanes, high, low):
        high_ref[:, lanes] = high
        low_ref[:, lanes] = low

    grad_block(unit, pl.program_id(0), refs[:-3], probs_ref, store)


def logit_grad(logits, routed, stats, counts, keep_mask, unit):
    rows, experts = logits.shape
    blocks = rows // LANES
    wide = pl.BlockSpec((LANES, experts), lambda i: (i, 0))
    thin = pl.BlockSpec((blocks, LANES), lambda i: (0, 0))
    flat = pl.BlockSpec((1, experts), lambda i: (0, 0))
    return pl.pallas_call(
        functools.partial(grad_kernel, unit),
        grid=(blocks,),
        in_specs=[wide, thin, thin, thin, thin, flat, flat],
        out_specs=[wide, wide],
        out_shape=[jax.ShapeDtypeStruct((rows, experts), jnp.bfloat16)] * 2,
        scratch_shapes=[pltpu.VMEM((LANES, experts), jnp.float32)],
        cost_estimate=pl.CostEstimate(
            flops=20 * rows * experts, bytes_accessed=8 * rows * experts, transcendentals=0
        ),
        name="logit_grad",
    )(logits, routed, *stats, counts, keep_mask)


class Walk:
    def __init__(self, half, core, lefts, experts, cols, zblocks, shift):
        self.half, self.core, self.shift = half, core, shift
        self.cols, self.experts, self.zblocks = cols, experts, zblocks
        self.rows = [left.shape[0] // zblocks for left in lefts]
        self.tokens = lefts[0].shape[1]

    def place(self, s):
        s = jnp.maximum(s - self.shift, 0)
        half = self.half
        low = jnp.where(s < 2, half, 1 - half)
        high = jnp.where(jnp.logical_or(s == 0, s == 3), 1 - half, half)
        return low, high

    def block_of(self, s, me):
        low, high = self.place(s)
        return jnp.bitwise_xor(me, self.core + 2 * low + 4 * high)

    def left_specs(self):
        full = [pl.BlockSpec((self.zblocks * r, self.tokens), lambda s, me: (0, 0)) for r in self.rows[:2]]
        part = pl.BlockSpec(
            (self.zblocks // 2 * self.rows[2], self.tokens), lambda s, me, half=self.half: (half, 0)
        )
        return full + [part]

    def out_specs(self):
        half, shift = self.half, self.shift
        deep = self.zblocks // 2

        def first(s, me):
            return (0, jnp.where(s - shift < 1, 1 - half, half), 0, 0, 0)

        def second(s, me):
            return (jnp.where(s - shift < 2, half, 1 - half), 0, 0, 0, 0)

        def third(s, me):
            low, high = self.place(s)
            return (high, low, 0, 0, 0)

        return [
            pl.BlockSpec((2, 1, deep, self.rows[0], self.cols), first),
            pl.BlockSpec((1, 2, deep, self.rows[1], self.cols), second),
            pl.BlockSpec((1, 1, deep, self.rows[2], self.cols), third),
        ]

    def out_shapes(self):
        return [
            jax.ShapeDtypeStruct((2, 2, self.zblocks // 2, r, self.cols), jnp.float32) for r in self.rows
        ]

    def multiply(self, s, lefts, high, low, outs, addends):
        s = s - self.shift

        def one(c):
            left = lefts[c][...]
            acc = jnp.dot(left, high(), preferred_element_type=jnp.float32)
            acc += jnp.dot(left, low(), preferred_element_type=jnp.float32)
            acc = acc.reshape(outs[c].shape)
            outs[c][...] = acc + addends[c][...] if addends else acc

        pl.when(jnp.logical_and(s >= 0, s < 2))(functools.partial(one, 0))
        pl.when(jnp.logical_and(s >= 1, s < 3))(functools.partial(one, 1))
        pl.when(s >= 0)(functools.partial(one, 2))

    def flops(self):
        return 4 * self.tokens * self.cols * self.zblocks * 2 * sum(self.rows)


def walk_kernel(walk, add, me_ref, a_ref, b_ref, c_ref, high_ref, low_ref, *rest):
    walk.multiply(
        pl.program_id(0),
        (a_ref, b_ref, c_ref),
        lambda: high_ref[...],
        lambda: low_ref[...],
        rest[-3:],
        rest[:3] if add else (),
    )


def products(half, core, lefts, high, low, me, expert_blocks, zblocks, addends=()):
    tokens, experts = high.shape
    cols = experts // expert_blocks
    walk = Walk(half, core, lefts, experts, cols, zblocks, 0)
    column = pl.BlockSpec((tokens, cols), lambda s, me: (0, walk.block_of(s, me[0])))
    outs = walk.out_specs()
    return pl.pallas_call(
        functools.partial(walk_kernel, walk, bool(addends)),
        grid_spec=pltpu.PrefetchScalarGridSpec(
            num_scalar_prefetch=1,
            grid=(4,),
            in_specs=walk.left_specs() + [column, column] + (outs if addends else []),
            out_specs=outs,
        ),
        out_shape=walk.out_shapes(),
        cost_estimate=pl.CostEstimate(
            flops=walk.flops(), bytes_accessed=4 * tokens * cols * 4 * 3, transcendentals=0
        ),
        name="products",
    )(me, *lefts, high, low, *addends)


def lead_kernel(walk, unit, blocks, me_ref, *refs):
    sources, lefts, (high_ref, low_ref), outs, (high_all, low_all, probs_ref) = (
        refs[:7], refs[7:10], refs[10:12], refs[12:15], refs[15:]
    )
    s = pl.program_id(0)

    @pl.when(s < blocks)
    def _():
        place = pl.ds(pl.multiple_of(s * LANES, LANES), LANES)

        def store(lanes, high, low):
            high_ref[:, lanes] = high
            low_ref[:, lanes] = low
            high_all[place, lanes] = high
            low_all[place, lanes] = low

        grad_block(unit, s, sources, probs_ref, store)

    low_bit, high_bit = walk.place(s)
    column = jnp.bitwise_xor(me_ref[0], walk.core + 2 * low_bit + 4 * high_bit)
    span = pl.ds(pl.multiple_of(column * walk.cols, LANES), walk.cols)
    walk.multiply(
        s,
        lefts,
        lambda: high_all[:, span],
        lambda: low_all[:, span],
        outs,
        (),
    )


def lead(logits, routed, stats, counts, keep_mask, unit, lefts, me, expert_blocks, zblocks):
    rows, experts = logits.shape
    blocks = rows // LANES
    cols = experts // expert_blocks
    walk = Walk(1, 1, lefts, experts, cols, zblocks, blocks)

    def row_block(s, me):
        return (jnp.minimum(s, blocks - 1), 0)

    wide = pl.BlockSpec((LANES, experts), row_block)
    thin = pl.BlockSpec((blocks, LANES), lambda s, me: (0, 0))
    flat = pl.BlockSpec((1, experts), lambda s, me: (0, 0))
    return pl.pallas_call(
        functools.partial(lead_kernel, walk, unit, blocks),
        grid_spec=pltpu.PrefetchScalarGridSpec(
            num_scalar_prefetch=1,
            grid=(blocks + 4,),
            in_specs=[wide, thin, thin, thin, thin, flat, flat] + walk.left_specs(),
            out_specs=[wide, wide] + walk.out_specs(),
            scratch_shapes=[pltpu.VMEM((rows, experts), jnp.bfloat16)] * 2
            + [pltpu.VMEM((LANES, experts), jnp.float32)],
        ),
        out_shape=[jax.ShapeDtypeStruct((rows, experts), jnp.bfloat16)] * 2 + walk.out_shapes(),
        cost_estimate=pl.CostEstimate(
            flops=walk.flops() + 2000 * rows * experts, bytes_accessed=12 * rows * experts, transcendentals=0
        ),
        name="lead",
    )(me, logits, routed, *stats, counts, keep_mask, *lefts)


def split_rows(rows, parts):
    tiles = rows // SUBLANES
    sizes = [tiles // parts + (1 if p < tiles % parts else 0) for p in range(parts)]
    return [s * SUBLANES for s in sizes]


def fits(tokens, router_logits):
    dp_width, expert_width = widths()
    rows, width = tokens.shape
    experts = router_logits.shape[1]
    bits = [w.bit_length() - 1 for w in (dp_width, expert_width)]
    powers = all(w == 1 << b for w, b in zip((dp_width, expert_width), bits))
    return (
        powers
        and bits[1] == 1 + 2
        and bits[0] == 2
        and width % (dp_width * SUBLANES) == 0
        and width // dp_width >= 3 * SUBLANES
        and experts % (expert_width * LANES) == 0
        and rows % LANES == 0
    )


def fallback(tokens, router_logits, gate_grad, expert_index, keep_mask, counts_here, unit):
    experts = router_logits.shape[1]
    counts = lax.psum(counts_here, ("dp", "expert")).reshape(1, experts)
    stats = softmax(router_logits, expert_index, gate_grad)
    high, low = logit_grad(router_logits, expert_index, stats, counts, keep_mask, unit)
    dims = (((0,), (0,)), ((), ()))
    partial = lax.dot_general(high, tokens, dims, preferred_element_type=jnp.float32)
    partial += lax.dot_general(low, tokens, dims, preferred_element_type=jnp.float32)
    owned = lax.psum_scatter(partial, "expert", scatter_dimension=0, tiled=True)
    return lax.psum_scatter(owned, "dp", scatter_dimension=1, tiled=True)


def local(tokens, router_logits, gate_grad, expert_index, keep_mask):
    dp_width, expert_width = widths()
    rows, width = tokens.shape
    experts = router_logits.shape[1]
    unit = experts / (rows * dp_width * expert_width)
    counts_here = local_counts(expert_index[:, 0], experts)
    expert_index = expert_index.reshape(rows // LANES, LANES)
    gate_grad = gate_grad.reshape(rows // LANES, LANES)
    keep_mask = keep_mask.reshape(1, experts)
    if not fits(tokens, router_logits):
        return fallback(tokens, router_logits, gate_grad, expert_index, keep_mask, counts_here, unit)

    counts = global_counts(counts_here).reshape(1, experts)
    stats = softmax(router_logits, expert_index, gate_grad)
    me = lax.axis_index("expert").astype(jnp.int32).reshape(1)
    me_dp = lax.axis_index("dp")
    zrows = width // dp_width
    low_bit, high_bit, near, far = ("expert", 1), ("expert", 2), ("dp", 0), ("dp", 1)
    orders = [
        (low_bit, near, high_bit, far),
        (high_bit, low_bit, near, far),
        (near, high_bit, low_bit, far),
    ]
    sizes = split_rows(zrows, len(orders))
    places = [near_bit + 2 * far_bit for near_bit in range(2) for far_bit in range(2)]
    pieces = [lax.dynamic_slice_in_dim(tokens, (me_dp ^ p) * zrows, zrows, 1).T for p in places]
    lefts = []
    offset = 0
    for size in sizes:
        lefts.append(jnp.concatenate([p[offset : offset + size] for p in pieces], axis=0))
        offset += size

    shared = dict(me=me, expert_blocks=expert_width, zblocks=dp_width)
    high, low, *away = lead(router_logits, expert_index, stats, counts, keep_mask, unit, lefts, **shared)
    arrived = [exchange(a, "expert", 1) for a in away]
    own = products(1, 0, lefts, high, low, **shared)
    sends = [o + r for o, r in zip(own, arrived)]
    sends, high, low = lax.optimization_barrier((sends, high, low))
    away = products(0, 1, lefts, high, low, **shared)
    rest = products(0, 0, lefts, high, low, addends=[exchange(a, "expert", 1) for a in away], **shared)
    held = [[r] for r in rest]
    for stage in range(len(orders[0])):
        for c, order in enumerate(orders):
            axis, bit = order[stage]
            held[c].append(exchange(sends[c], axis, 1 << bit))
        if stage == len(orders[0]) - 1:
            break
        for c in range(len(orders)):
            sends[c] = sum(h[1] for h in held[c][1:]) + held[c][0][1]
            held[c] = [h[0] for h in held[c]]
    out = jnp.concatenate([sum(h[1:], h[0]) for h in held], axis=0)
    return out.T


def solution(mesh):
    in_specs = (
        P(("dp", "expert"), None),
        P(("dp", "expert"), None),
        P(("dp", "expert")),
        P(("dp", "expert"), None),
        P(),
    )
    out_specs = P("expert", "dp")
    return jax.shard_map(local, mesh=mesh, in_specs=in_specs, out_specs=out_specs, check_vma=False)
```
